32 devices in a mesh: py: 4 (over y, core), pz: 8 (over z, x).
Axes of the slice: x: 2, y: 2, z: 4, core: 2. Of those that a mesh axis runs over, the one named last changes fastest.
Arguments:
- wavefunctions: float32 [2, 8, 128, 128, 128], P(None, None, 'pz', 'py'), may hold values from -6 to 6
- potential: float32 [128, 128, 128], P('pz', 'py'), may hold values from -4 to 4
- cutoff_sq: int32 [1], replicated, may hold values from 2304 to 4096
- locked_mask: int32 [8], replicated, may hold values 0 or 1
Outputs:
- applied: float32 [2, 8, 128, 128, 128], P(None, None, 'pz', 'py')
- rayleigh: float32 [8], replicated
- residual_norm: float32 [8], replicated
The draws below stay inside these ranges and needn't reach their ends.
All inputs are finite; a program needn't handle non-finite values.
Results may differ from the reference program's by a relative error of at most 0.00005.
Values sent between devices are 32-bit elements; how exact they have to be, the bound alone decides.
No kernel may reach another device: no remote copies, remote signals or barrier semaphores. Data moves between devices by JAX's collectives and lax.ppermute only.
A program may use at most 64 MiB of HBM per device.

```python
import math
import jax
import jax.numpy as jnp
from jax import lax

GRID = 128
NB = 8


def place_ends(entries, own_key, least, largest):
    extent = entries.shape
    place = [jax.random.randint(jax.random.fold_in(own_key, axis), (), 0, extent[axis]) for axis in range(len(extent))]
    entries = entries.at[tuple(place)].set(least)
    longest = extent.index(max(extent))
    place[longest] = (place[longest] + 1) % extent[longest]
    return entries.at[tuple(place)].set(largest)


def steps_of(stream_key, dims, pieces, smallest, top_value):
    def one(dim, parts):
        draws = jax.random.uniform(jax.random.fold_in(jax.random.fold_in(stream_key, 6), dim), (parts,), jnp.float32, smallest / len(pieces), top_value / len(pieces))
        return jnp.repeat(jnp.exp(draws), dims[dim] // parts).reshape((-1,) + (1,) * (len(dims) - dim - 1))

    level = one(*pieces[0])
    for cut in pieces[1:]:
        level = level * one(*cut)
    return level


def centred(rng, extent, scale, limit, shards=(), held_as=jnp.bfloat16):
    result = jax.random.normal(rng, extent, jnp.float32) * scale
    if len(shards) > 0:
        result = steps_of(rng, extent, shards, -0.22, 0.18) * result
    return jnp.clip(result, min=-limit, max=limit).astype(held_as)


def setup_inputs(seed: int = 0) -> dict:
    keys = jax.random.split(jax.random.key(seed), 5)
    return {
        "wavefunctions": centred(keys[0], (2, NB, GRID, GRID, GRID), 1.0, 6.0, ((2, 8), (3, 4)), jnp.float32),
        "potential": centred(keys[1], (GRID, GRID, GRID), 1.0, 4.0, ((0, 8), (1, 4)), jnp.float32),
        "cutoff_sq": jax.random.randint(keys[2], (1,), GRID * GRID * 9 // 64, GRID * GRID // 4 + 1).astype(jnp.int32),
        "locked_mask": place_ends((jax.random.randint(keys[3], (NB,), 0, 4) < 1).astype(jnp.int32), jax.random.fold_in(keys[3], 1), 0, 1),
    }


def reference(wavefunctions, potential, cutoff_sq, locked_mask):
    freq = jnp.arange(GRID, dtype=jnp.int32)
    signed = jnp.where(freq < GRID // 2, freq, freq - GRID)
    square = signed * signed
    total = square[:, None, None] + square[None, :, None] + square[None, None, :]
    keep = (total <= cutoff_sq[0]).astype(jnp.float32)
    kinetic = 0.5 * (math.pi / GRID) ** 2 * total.astype(jnp.float32) * keep

    def one_band(pair):
        real_part, imag_part = pair
        field = real_part + 1j * imag_part
        spectrum = jnp.fft.fftn(field)
        back = jnp.fft.ifftn(spectrum * kinetic)
        return (jnp.real(back) + potential * real_part, jnp.imag(back) + potential * imag_part)
    applied_real, applied_imag = lax.map(one_band, (wavefunctions[0], wavefunctions[1]))
    applied = jnp.stack([applied_real, applied_imag])
    norm_sq = lax.optimization_barrier(jnp.sum(wavefunctions * wavefunctions, axis=(0, 2, 3, 4)))
    correlation = lax.optimization_barrier(jnp.sum(wavefunctions * applied, axis=(0, 2, 3, 4)))
    rayleigh = correlation / norm_sq
    residual = applied - rayleigh[None, :, None, None, None] * wavefunctions
    residual_sq = lax.optimization_barrier(jnp.sum(residual * residual, axis=(0, 2, 3, 4)))
    residual_norm = jnp.sqrt(residual_sq / norm_sq) * (1.0 - locked_mask.astype(jnp.float32))
    return (applied, rayleigh, residual_norm)
```

```python
import functools
import math

import jax
import jax.numpy as jnp
import ml_dtypes
import numpy as np
from jax import lax
from jax.experimental import pallas as pl
from jax.experimental.pallas import tpu as pltpu
from jax.sharding import PartitionSpec as P

F32 = jnp.float32
BF16 = jnp.bfloat16


def split_table(length, inverse):
    counter = np.arange(length)
    angle = 2.0 * np.pi / length * (counter[:, None] * counter[None, :] % length)
    scale = 1.0 / length if inverse else 1.0
    sign = 1.0 if inverse else -1.0
    cosines, sines = scale * np.cos(angle), sign * scale * np.sin(angle)
    table = np.block([[cosines, -sines], [sines, cosines]]).astype(np.float32)
    high = table.astype(ml_dtypes.bfloat16)
    low = (table - high.astype(np.float32)).astype(ml_dtypes.bfloat16)
    return high, low


def split(value):
    high = value.astype(BF16)
    return high, (value - high.astype(F32)).astype(BF16)


def dot(left, right):
    return jnp.dot(left, right, preferred_element_type=F32)


def left_apply(high, low, value):
    vh, vl = split(value)
    return dot(high, vh) + (dot(high, vl) + dot(low, vh))


def right_apply(value, high, low):
    vh, vl = split(value)
    return dot(vh, high) + (dot(vl, high) + dot(vh, low))


def forward_kernel(lh, ll, rh, rl, src, dst):
    pieces, _, depth, rows, n = src.shape
    owners, width = dst.shape[0], dst.shape[3]
    planes = []
    for z in range(depth):
        part = [
            jnp.concatenate([src[s, p, z] for s in range(pieces)], axis=0) for p in range(2)
        ]
        planes.append(jnp.concatenate(part, axis=1))
    along_x = right_apply(jnp.concatenate(planes, axis=0), rh[...], rl[...])
    columns = jnp.concatenate(
        [
            jnp.concatenate(
                [along_x[z * n : (z + 1) * n, :n], along_x[z * n : (z + 1) * n, n:]], axis=0
            )
            for z in range(depth)
        ],
        axis=1,
    )
    out = left_apply(lh[...], ll[...], columns)
    for z in range(depth):
        for q in range(2):
            for d in range(owners):
                first = q * n + d * width
                dst[d, q, z] = out[first : first + width, z * n : (z + 1) * n]


def middle_kernel(scalars, fh, fl, ih, il, src, dst):
    owners, _, depth, width, n = src.shape
    planes = []
    for q in range(2):
        planes.append(jnp.swapaxes(src[:, q].reshape(owners * depth, width, n), 0, 1))
    columns = jnp.concatenate(
        [jnp.concatenate([planes[0][j], planes[1][j]], axis=0) for j in range(width)], axis=1
    )
    spectrum = left_apply(fh[...], fl[...], columns)
    kz = lax.broadcasted_iota(jnp.int32, (n, n), 0)
    kx = lax.broadcasted_iota(jnp.int32, (n, n), 1)
    kz = jnp.where(kz < n // 2, kz, kz - n)
    kx = jnp.where(kx < n // 2, kx, kx - n)
    base = kz * kz + kx * kx
    cutoff = scalars[0]
    start = scalars[1] + pl.program_id(0) * width
    kinetic = []
    for j in range(width):
        ky = start + j
        ky = jnp.where(ky < n // 2, ky, ky - n)
        total = base + ky * ky
        value = (0.5 * (math.pi / n) ** 2) * total.astype(F32)
        kinetic.append(jnp.where(total <= cutoff, value, 0.0))
    kinetic = jnp.concatenate(kinetic, axis=1)
    kinetic = jnp.concatenate([kinetic, kinetic], axis=0)
    back = left_apply(ih[...], il[...], spectrum * kinetic)
    for q in range(2):
        stacked = jnp.stack(
            [back[q * n : (q + 1) * n, j * n : (j + 1) * n] for j in range(width)], axis=0
        )
        dst[:, q] = jnp.swapaxes(stacked, 0, 1).reshape(owners, depth, width, n)


def whole(shape):
    return pl.BlockSpec(shape, lambda i: (0,) * len(shape))


PARAMS = dict(dimension_semantics=("arbitrary",), vmem_limit_bytes=40 * 1024 * 1024)


def planes_call(left, right, src, out_shape):
    depth = math.gcd(src.shape[2], 4)
    n = src.shape[4]

    def spec(shape):
        return pl.BlockSpec((shape[0], 2, depth, shape[3], n), lambda i: (0, 0, i, 0, 0))

    table = whole((2 * n, 2 * n))
    return pl.pallas_call(
        forward_kernel,
        grid=(src.shape[2] // depth,),
        in_specs=[table] * 4 + [spec(src.shape)],
        out_specs=spec(out_shape),
        out_shape=jax.ShapeDtypeStruct(out_shape, F32),
        compiler_params=pltpu.CompilerParams(**PARAMS),
    )(*left, *right, src)


def middle_call(scalars, forward, inverse, src):
    owners, _, depth, rows, n = src.shape
    width = min(8, rows)
    block = pl.BlockSpec((owners, 2, depth, width, n), lambda i: (0, 0, 0, i, 0))
    table = whole((2 * n, 2 * n))
    return pl.pallas_call(
        middle_kernel,
        grid=(rows // width,),
        in_specs=[pl.BlockSpec(memory_space=pltpu.SMEM)] + [table] * 4 + [block],
        out_specs=block,
        out_shape=jax.ShapeDtypeStruct(src.shape, F32),
        compiler_params=pltpu.CompilerParams(**PARAMS),
    )(scalars, *forward, *inverse, src)


def finish_kernel(kin, wave, pot, out, stats):
    parts = []
    norm = corr = 0.0
    for p in range(2):
        w = wave[p, 0]
        a = kin[0, p] + pot[...] * w
        out[p, 0] = a
        norm = norm + jnp.sum(jnp.sum(w * w, axis=0), keepdims=True)
        corr = corr + jnp.sum(jnp.sum(w * a, axis=0), keepdims=True)
    ratio = jnp.where(norm > 0.0, corr / jnp.where(norm > 0.0, norm, 1.0), 0.0)
    rest = 0.0
    for p in range(2):
        gap = out[p, 0] - ratio[None] * wave[p, 0]
        rest = rest + jnp.sum(jnp.sum(gap * gap, axis=0), keepdims=True)
    row = lax.broadcasted_iota(jnp.int32, stats.shape[1:], 0)
    stats[0] = jnp.where(row == 0, norm, jnp.where(row == 1, corr, rest))


def finish_call(kin, wave, pot):
    _, bands, depth, rows, n = wave.shape
    band = pl.BlockSpec((2, 1, depth, rows, n), lambda i: (0, i, 0, 0, 0))
    return pl.pallas_call(
        finish_kernel,
        grid=(bands,),
        in_specs=[
            pl.BlockSpec((1, 2, depth, rows, n), lambda i: (i, 0, 0, 0, 0)),
            band,
            whole(pot.shape),
        ],
        out_specs=[band, pl.BlockSpec((1, 8, 128), lambda i: (i, 0, 0))],
        out_shape=[
            jax.ShapeDtypeStruct(wave.shape, F32),
            jax.ShapeDtypeStruct((bands, 8, 128), F32),
        ],
        compiler_params=pltpu.CompilerParams(**PARAMS),
    )(kin, wave, pot)


def exchange(value, axis):
    return lax.all_to_all(value, axis, split_axis=0, concat_axis=0, tiled=True)


def body(wavefunctions, potential, cutoff_sq, locked_mask):
    _, bands, rows_z, rows_y, n = wavefunctions.shape
    size_y, size_z = lax.axis_size("py"), lax.axis_size("pz")
    fh, fl = split_table(n, False)
    ih, il = split_table(n, True)
    fwd, inv = (fh, fl), (ih, il)
    fwd_t = (np.ascontiguousarray(fh.T), np.ascontiguousarray(fl.T))
    inv_t = (np.ascontiguousarray(ih.T), np.ascontiguousarray(il.T))
    share = n // size_z
    scalars = jnp.stack([cutoff_sq[0], (lax.axis_index("pz") * share).astype(jnp.int32)])
    pieces = []
    for first in range(0, bands, size_y):
        pieces.append(jnp.swapaxes(wavefunctions[:, first : first + size_y], 0, 1))
    pieces = [exchange(piece, "py") for piece in pieces]
    pieces = [planes_call(fwd, fwd_t, x, (size_z, 2, rows_z, share, n)) for x in pieces]
    pieces = [exchange(piece, "pz") for piece in pieces]
    pieces = [middle_call(scalars, fwd, inv, x) for x in pieces]
    pieces = [exchange(piece, "pz") for piece in pieces]
    pieces = [planes_call(inv, inv_t, x, (size_y, 2, rows_z, rows_y, n)) for x in pieces]
    pieces = [exchange(piece, "py") for piece in pieces]
    kinetic_part = jnp.concatenate(pieces, axis=0)
    applied, stats = finish_call(kinetic_part, wavefunctions, potential)
    local = stats[:, :3, 0].T
    every = lax.all_gather(local.reshape(1, 3 * bands), ("py", "pz"), axis=0, tiled=True)
    norm, corr, rest = jnp.split(every, 3, axis=1)
    norm_sq = jnp.sum(norm, axis=0)
    rayleigh = jnp.sum(corr, axis=0) / norm_sq
    ratio = jnp.where(norm > 0.0, corr / jnp.where(norm > 0.0, norm, 1.0), 0.0)
    shift = ratio - rayleigh[None]
    residual_sq = jnp.sum(rest + shift * shift * norm, axis=0)
    residual_norm = jnp.sqrt(residual_sq / norm_sq) * (1.0 - locked_mask.astype(F32))
    return (applied, rayleigh, residual_norm)


def solution(mesh):
    in_specs = (P(None, None, "pz", "py", None), P("pz", "py", None), P(), P())
    out_specs = (P(None, None, "pz", "py", None), P(), P())
    return jax.shard_map(body, mesh=mesh, in_specs=in_specs, out_specs=out_specs, check_vma=False)
```

```python
import math

import jax
import jax.numpy as jnp
import ml_dtypes
import numpy as np
from jax import lax
from jax.experimental import pallas as pl
from jax.experimental.pallas import tpu as pltpu
from jax.sharding import PartitionSpec as P

F32 = jnp.float32
BF16 = jnp.bfloat16


def split_table(length, inverse):
    counter = np.arange(length)
    angle = 2.0 * np.pi / length * (counter[:, None] * counter[None, :] % length)
    scale = 1.0 / length if inverse else 1.0
    sign = 1.0 if inverse else -1.0
    cosines, sines = scale * np.cos(angle), sign * scale * np.sin(angle)
    table = np.block([[cosines, -sines], [sines, cosines]]).astype(np.float32)
    high = table.astype(ml_dtypes.bfloat16)
    low = (table - high.astype(np.float32)).astype(ml_dtypes.bfloat16)
    return high, low


def split(value):
    high = value.astype(BF16)
    return high, (value - high.astype(F32)).astype(BF16)


def dot(left, right):
    return jnp.dot(left, right, preferred_element_type=F32)


def left_apply(high, low, value):
    vh, vl = split(value)
    return dot(high, vh) + (dot(high, vl) + dot(low, vh))


def right_apply(value, high, low):
    vh, vl = split(value)
    return dot(vh, high) + (dot(vl, high) + dot(vh, low))


def planes_kernel(order, lh, ll, rh, rl, src, dst):
    pieces, _, depth, rows, n = src.shape
    owners, width = dst.shape[0], dst.shape[3]
    planes = []
    for z in range(depth):
        part = [
            jnp.concatenate([src[s ^ order[0], p, z] for s in range(pieces)], axis=0)
            for p in range(2)
        ]
        planes.append(jnp.concatenate(part, axis=1))
    along_x = right_apply(jnp.concatenate(planes, axis=0), rh[...], rl[...])
    columns = jnp.concatenate(
        [
            jnp.concatenate(
                [along_x[z * n : (z + 1) * n, :n], along_x[z * n : (z + 1) * n, n:]], axis=0
            )
            for z in range(depth)
        ],
        axis=1,
    )
    out = left_apply(lh[...], ll[...], columns)
    for z in range(depth):
        for q in range(2):
            for d in range(owners):
                first = q * n + d * width
                dst[d ^ order[1], q, z] = out[first : first + width, z * n : (z + 1) * n]


def middle_kernel(scalars, fh, fl, ih, il, src, dst):
    owners, _, depth, width, n = src.shape
    planes = []
    for q in range(2):
        planes.append(jnp.swapaxes(src[:, q].reshape(owners * depth, width, n), 0, 1))
    columns = jnp.concatenate(
        [jnp.concatenate([planes[0][j], planes[1][j]], axis=0) for j in range(width)], axis=1
    )
    spectrum = left_apply(fh[...], fl[...], columns)
    kz = lax.broadcasted_iota(jnp.int32, (n, n), 0)
    kx = lax.broadcasted_iota(jnp.int32, (n, n), 1)
    kz = jnp.where(kz < n // 2, kz, kz - n)
    kx = jnp.where(kx < n // 2, kx, kx - n)
    base = kz * kz + kx * kx
    cutoff = scalars[0]
    start = scalars[1] + pl.program_id(0) * width
    kinetic = []
    for j in range(width):
        ky = start + j
        ky = jnp.where(ky < n // 2, ky, ky - n)
        total = base + ky * ky
        value = (0.5 * (math.pi / n) ** 2) * total.astype(F32)
        kinetic.append(jnp.where(total <= cutoff, value, 0.0))
    kinetic = jnp.concatenate(kinetic, axis=1)
    kinetic = jnp.concatenate([kinetic, kinetic], axis=0)
    back = left_apply(ih[...], il[...], spectrum * kinetic)
    for q in range(2):
        stacked = jnp.stack(
            [back[q * n : (q + 1) * n, j * n : (j + 1) * n] for j in range(width)], axis=0
        )
        dst[:, q] = jnp.swapaxes(stacked, 0, 1).reshape(owners, depth, width, n)


def whole(shape):
    return pl.BlockSpec(shape, lambda i: (0,) * len(shape))


PARAMS = dict(dimension_semantics=("arbitrary",), vmem_limit_bytes=40 * 1024 * 1024)


def planes_call(order, left, right, src, out_shape):
    depth = math.gcd(src.shape[2], 4)
    n = src.shape[4]

    def spec(shape):
        return pl.BlockSpec((shape[0], 2, depth, shape[3], n), lambda i: (0, 0, i, 0, 0))

    table = whole((2 * n, 2 * n))
    return pl.pallas_call(
        planes_kernel,
        grid=(src.shape[2] // depth,),
        in_specs=[pl.BlockSpec(memory_space=pltpu.SMEM)] + [table] * 4 + [spec(src.shape)],
        out_specs=spec(out_shape),
        out_shape=jax.ShapeDtypeStruct(out_shape, F32),
        compiler_params=pltpu.CompilerParams(**PARAMS),
    )(order, *left, *right, src)


def middle_call(scalars, forward, inverse, src):
    owners, _, depth, rows, n = src.shape
    width = min(8, rows)
    block = pl.BlockSpec((owners, 2, depth, width, n), lambda i: (0, 0, 0, i, 0))
    table = whole((2 * n, 2 * n))
    return pl.pallas_call(
        middle_kernel,
        grid=(rows // width,),
        in_specs=[pl.BlockSpec(memory_space=pltpu.SMEM)] + [table] * 4 + [block],
        out_specs=block,
        out_shape=jax.ShapeDtypeStruct(src.shape, F32),
        compiler_params=pltpu.CompilerParams(**PARAMS),
    )(scalars, *forward, *inverse, src)


def finish_kernel(me, kin, wave, pot, *refs):
    out, stats = refs[-2:]
    norm = corr = 0.0
    for p in range(2):
        w = wave[p, 0]
        a = kin[0, p] + pot[...] * w
        out[p, 0] = a
        norm = norm + jnp.sum(jnp.sum(w * w, axis=0), keepdims=True)
        corr = corr + jnp.sum(jnp.sum(w * a, axis=0), keepdims=True)
    ratio = jnp.where(norm > 0.0, corr / jnp.where(norm > 0.0, norm, 1.0), 0.0)
    rest = 0.0
    for p in range(2):
        gap = out[p, 0] - ratio[None] * wave[p, 0]
        rest = rest + jnp.sum(jnp.sum(gap * gap, axis=0), keepdims=True)
    row = lax.broadcasted_iota(jnp.int32, stats.shape[1:], 0)
    stats[0] = jnp.where(row == 0, norm, jnp.where(row == 1, corr, rest))


def finish_call(me, kin, wave, pot, first, applied):
    _, bands, depth, rows, n = wave.shape
    count = kin.shape[0]
    band = pl.BlockSpec((2, 1, depth, rows, n), lambda i, me: (0, first + (i ^ me[0]), 0, 0, 0))
    in_specs = [
        pl.BlockSpec((1, 2, depth, rows, n), lambda i, me: (i, 0, 0, 0, 0)),
        band,
        pl.BlockSpec(pot.shape, lambda i, me: (0, 0, 0)),
    ]
    args, aliases = [me, kin, wave, pot], {}
    if applied is not None:
        in_specs.append(pl.BlockSpec(memory_space=pl.ANY))
        args.append(applied)
        aliases = {4: 0}
    return pl.pallas_call(
        finish_kernel,
        grid_spec=pltpu.PrefetchScalarGridSpec(
            num_scalar_prefetch=1,
            grid=(count,),
            in_specs=in_specs,
            out_specs=[band, pl.BlockSpec((1, 8, 128), lambda i, me: (i ^ me[0], 0, 0))],
        ),
        out_shape=[
            jax.ShapeDtypeStruct(wave.shape, F32),
            jax.ShapeDtypeStruct((count, 8, 128), F32),
        ],
        input_output_aliases=aliases,
        compiler_params=pltpu.CompilerParams(**PARAMS),
    )(*args)


def exchange(value, axis):
    return lax.all_to_all(value, axis, split_axis=0, concat_axis=0, tiled=True)


def swap(pieces, axis):
    size = len(pieces)
    return jnp.stack(
        [pieces[0]]
        + [
            lax.ppermute(pieces[d], axis, [(i, i ^ d) for i in range(size)])
            for d in range(1, size)
        ]
    )


def merge(stats, axis):
    size = lax.axis_size(axis)
    every = exchange(jnp.broadcast_to(stats[None], (size,) + stats.shape), axis)
    norm, corr, rest = every[:, 0], every[:, 1], every[:, 2]
    norm_all, corr_all = jnp.sum(norm, axis=0), jnp.sum(corr, axis=0)
    gap = ratio_of(corr, norm) - ratio_of(corr_all, norm_all)[None]
    return jnp.stack([norm_all, corr_all, jnp.sum(rest + gap * gap * norm, axis=0)])


def ratio_of(corr, norm):
    return jnp.where(norm > 0.0, corr / jnp.where(norm > 0.0, norm, 1.0), 0.0)


def body(wavefunctions, potential, cutoff_sq, locked_mask):
    _, bands, rows_z, rows_y, n = wavefunctions.shape
    size_y, size_z = lax.axis_size("py"), lax.axis_size("pz")
    fh, fl = split_table(n, False)
    ih, il = split_table(n, True)
    fwd, inv = (fh, fl), (ih, il)
    fwd_t = (np.ascontiguousarray(fh.T), np.ascontiguousarray(fl.T))
    inv_t = (np.ascontiguousarray(ih.T), np.ascontiguousarray(il.T))
    share = n // size_z
    scalars = jnp.stack([cutoff_sq[0], (lax.axis_index("pz") * share).astype(jnp.int32)])
    me = lax.axis_index("py").astype(jnp.int32)
    there, back = jnp.stack([me, 0 * me]), jnp.stack([0 * me, me])
    spectra = []
    gathered = None
    for first in range(0, bands, size_y):
        source = wavefunctions
        if gathered is not None:
            source, gathered = lax.optimization_barrier((source, gathered))
            spectra[-1] = gathered
        sent = [
            lax.dynamic_index_in_dim(source, first + (me ^ d), 1, keepdims=False)
            for d in range(size_y)
        ]
        gathered = swap(sent, "py")
        spectra.append(gathered)
    pieces = [planes_call(there, fwd, fwd_t, x, (size_z, 2, rows_z, share, n)) for x in spectra]
    pieces = [exchange(piece, "pz") for piece in pieces]
    pieces = [middle_call(scalars, fwd, inv, x) for x in pieces]
    pieces = [exchange(piece, "pz") for piece in pieces]
    pieces = [planes_call(back, inv, inv_t, x, (size_y, 2, rows_z, rows_y, n)) for x in pieces]
    applied, stats = None, []
    for index, piece in enumerate(pieces):
        kinetic_part = swap([piece[d] for d in range(size_y)], "py")
        applied, some = finish_call(
            me[None], kinetic_part, wavefunctions, potential, index * size_y, applied
        )
        stats.append(some[:, :3, 0])
    total = merge(merge(jnp.concatenate(stats, axis=0).T, "py"), "pz")
    rayleigh = total[1] / total[0]
    residual_norm = jnp.sqrt(total[2] / total[0]) * (1.0 - locked_mask.astype(F32))
    return (applied, rayleigh, residual_norm)


def solution(mesh):
    in_specs = (P(None, None, "pz", "py", None), P("pz", "py", None), P(), P())
    out_specs = (P(None, None, "pz", "py", None), P(), P())
    return jax.shard_map(body, mesh=mesh, in_specs=in_specs, out_specs=out_specs, check_vma=False)
```

```python
import math

import jax
import jax.numpy as jnp
import ml_dtypes
import numpy as np
from jax import lax
from jax.experimental import pallas as pl
from jax.experimental.pallas import tpu as pltpu
from jax.sharding import PartitionSpec as P

F32 = jnp.float32
BF16 = jnp.bfloat16


def split_table(length, inverse):
    counter = np.arange(length)
    angle = 2.0 * np.pi / length * (counter[:, None] * counter[None, :] % length)
    scale = 1.0 / length if inverse else 1.0
    sign = 1.0 if inverse else -1.0
    cosines, sines = scale * np.cos(angle), sign * scale * np.sin(angle)
    table = np.block([[cosines, -sines], [sines, cosines]]).astype(np.float32)
    high = table.astype(ml_dtypes.bfloat16)
    low = (table - high.astype(np.float32)).astype(ml_dtypes.bfloat16)
    return high, low


def split(value):
    high = value.astype(BF16)
    return high, (value - high.astype(F32)).astype(BF16)


def dot(left, right):
    return jnp.dot(left, right, preferred_element_type=F32)


def left_apply(high, low, value):
    vh, vl = split(value)
    return dot(high, vh) + (dot(high, vl) + dot(low, vh))


def right_apply(value, high, low):
    vh, vl = split(value)
    return dot(vh, high) + (dot(vl, high) + dot(vh, low))


def packing(n, owners):
    limit = n * n // 4
    signed = [k if k < n // 2 else k - n for k in range(n)]
    reach = [math.isqrt(limit - f * f) for f in signed]
    free, pairs = set(range(n)), []
    for tail in sorted(range(n), key=lambda k: reach[k]):
        fits = [k for k in free if k != tail and reach[k] + reach[tail] < n // 2]
        if tail in free and fits:
            host = max(fits, key=lambda k: reach[k])
            pairs.append((host, tail))
            free -= {host, tail}
    count = max(c for c in range(0, len(pairs) + 1, 8) if (n - c) % owners == 0)
    pairs = pairs[:count]
    used = {k for pair in pairs for k in pair}
    hosts, tails = [h for h, _ in pairs], [t for _, t in pairs]
    order = [k for k in range(n) if k not in used] + hosts + tails
    rows = n - count
    f = np.array(signed)
    square = (f[order[:rows], None] ** 2 + f[None, :] ** 2).astype(np.int32)
    own = np.ones((max(count, 8), n), np.int32)
    for i, (host, tail) in enumerate(pairs):
        lane = np.arange(n)
        own[i] = (lane <= reach[host]) | (lane >= n - reach[host])
        other = f[tail] ** 2 + np.roll(f, n // 2) ** 2
        square[rows - count + i] = np.where(own[i], square[rows - count + i], other)
    return np.array(order), rows, square, own


def gather_planes(planes):
    depth, n = len(planes), planes[0].shape[0]
    return lambda along: jnp.concatenate(
        [
            jnp.concatenate([along[z * n : (z + 1) * n, :n], along[z * n : (z + 1) * n, n:]], axis=0)
            for z in range(depth)
        ],
        axis=1,
    )


def forward_kernel(order, lh, ll, rh, rl, own, src, dst):
    pieces, _, depth, _, n = src.shape
    owners, _, share, _, _ = dst.shape
    rows = owners * share
    count = n - rows
    planes = []
    for z in range(depth):
        part = [
            jnp.concatenate([src[s ^ order[0], p, z] for s in range(pieces)], axis=0)
            for p in range(2)
        ]
        planes.append(jnp.concatenate(part, axis=1))
    along_x = right_apply(jnp.concatenate(planes, axis=0), rh[...], rl[...])
    out = left_apply(lh[...], ll[...], gather_planes(planes)(along_x))
    for q in range(2):
        packed = []
        for z in range(depth):
            plane = out[q * n : (q + 1) * n, z * n : (z + 1) * n]
            if count:
                tail = pltpu.roll(plane[rows:], n // 2, 1)
                host = jnp.where(own[...] != 0, plane[rows - count : rows], tail)
                plane = jnp.concatenate([plane[: rows - count], host], axis=0)
            packed.append(plane)
        packed = jnp.swapaxes(jnp.stack(packed, axis=0), 0, 1)
        dst[:, q] = packed.reshape(owners, share, depth, n)


def inverse_kernel(order, lh, ll, rh, rl, own, src, dst):
    owners, _, share, depth, n = src.shape
    pieces, _, _, width, _ = dst.shape
    rows = owners * share
    count = n - rows
    parts = [jnp.swapaxes(src[:, p].reshape(rows, depth, n), 0, 1) for p in range(2)]
    planes = []
    for z in range(depth):
        part = []
        for p in range(2):
            plane = parts[p][z]
            if count:
                last = plane[rows - count :]
                host = jnp.where(own[...] != 0, last, 0.0)
                tail = pltpu.roll(jnp.where(own[...] != 0, 0.0, last), n // 2, 1)
                plane = jnp.concatenate([plane[: rows - count], host, tail], axis=0)
            part.append(plane)
        planes.append(jnp.concatenate(part, axis=1))
    along_x = right_apply(jnp.concatenate(planes, axis=0), rh[...], rl[...])
    out = left_apply(lh[...], ll[...], gather_planes(planes)(along_x))
    for z in range(depth):
        for q in range(2):
            for d in range(pieces):
                first = q * n + d * width
                dst[d ^ order[1], q, z] = out[first : first + width, z * n : (z + 1) * n]


def middle_kernel(cutoff, squares, fh, fl, ih, il, src, dst):
    owners, _, width, depth, n = src.shape
    columns = jnp.concatenate(
        [
            jnp.concatenate([src[:, q, j].reshape(owners * depth, n) for q in range(2)], axis=0)
            for j in range(width)
        ],
        axis=1,
    )
    spectrum = left_apply(fh[...], fl[...], columns)
    kz = lax.broadcasted_iota(jnp.int32, (n, n), 0)
    kz = jnp.where(kz < n // 2, kz, kz - n)
    base = kz * kz
    kinetic = []
    for j in range(width):
        total = base + squares[j]
        value = (0.5 * (math.pi / n) ** 2) * total.astype(F32)
        kinetic.append(jnp.where(total <= cutoff[0], value, 0.0))
    kinetic = jnp.concatenate(kinetic, axis=1)
    kinetic = jnp.concatenate([kinetic, kinetic], axis=0)
    back = left_apply(ih[...], il[...], spectrum * kinetic)
    for q in range(2):
        for j in range(width):
            plane = back[q * n : (q + 1) * n, j * n : (j + 1) * n]
            dst[:, q, j] = plane.reshape(owners, depth, n)


def whole(shape):
    return pl.BlockSpec(shape, lambda i: (0,) * len(shape))


PARAMS = dict(dimension_semantics=("arbitrary",), vmem_limit_bytes=40 * 1024 * 1024)


def planes_call(kernel, order, left, right, own, src, out_shape, depths):
    n = src.shape[4]
    depth = math.gcd(src.shape[depths[0]], 8)

    def spec(shape, axis):
        block = shape[:axis] + (depth,) + shape[axis + 1 :]
        return pl.BlockSpec(block, lambda i: tuple(i if a == axis else 0 for a in range(5)))

    table = whole((2 * n, 2 * n))
    return pl.pallas_call(
        kernel,
        grid=(src.shape[depths[0]] // depth,),
        in_specs=[pl.BlockSpec(memory_space=pltpu.SMEM)]
        + [table] * 4
        + [whole(own.shape), spec(src.shape, depths[0])],
        out_specs=spec(out_shape, depths[1]),
        out_shape=jax.ShapeDtypeStruct(out_shape, F32),
        compiler_params=pltpu.CompilerParams(**PARAMS),
    )(order, *left, *right, own, src)


def middle_call(cutoff, squares, forward, inverse, src):
    owners, _, rows, depth, n = src.shape
    width = max(w for w in range(1, 9) if rows % w == 0)
    block = pl.BlockSpec((owners, 2, width, depth, n), lambda i: (0, 0, i, 0, 0))
    table = whole((2 * n, 2 * n))
    return pl.pallas_call(
        middle_kernel,
        grid=(rows // width,),
        in_specs=[
            pl.BlockSpec(memory_space=pltpu.SMEM),
            pl.BlockSpec((width, 1, n), lambda i: (i, 0, 0)),
        ]
        + [table] * 4
        + [block],
        out_specs=block,
        out_shape=jax.ShapeDtypeStruct(src.shape, F32),
        compiler_params=pltpu.CompilerParams(**PARAMS),
    )(cutoff, squares, *forward, *inverse, src)


def finish_kernel(me, kin, wave, pot, *refs):
    out, stats = refs[-2:]
    norm = corr = 0.0
    for p in range(2):
        w = wave[p, 0]
        a = kin[0, p] + pot[...] * w
        out[p, 0] = a
        norm = norm + jnp.sum(jnp.sum(w * w, axis=0), keepdims=True)
        corr = corr + jnp.sum(jnp.sum(w * a, axis=0), keepdims=True)
    ratio = jnp.where(norm > 0.0, corr / jnp.where(norm > 0.0, norm, 1.0), 0.0)
    rest = 0.0
    for p in range(2):
        gap = out[p, 0] - ratio[None] * wave[p, 0]
        rest = rest + jnp.sum(jnp.sum(gap * gap, axis=0), keepdims=True)
    row = lax.broadcasted_iota(jnp.int32, stats.shape[1:], 0)
    stats[0] = jnp.where(row == 0, norm, jnp.where(row == 1, corr, rest))


def finish_call(me, kin, wave, pot, first, applied):
    _, bands, depth, rows, n = wave.shape
    count = kin.shape[0]
    band = pl.BlockSpec((2, 1, depth, rows, n), lambda i, me: (0, first + (i ^ me[0]), 0, 0, 0))
    in_specs = [
        pl.BlockSpec((1, 2, depth, rows, n), lambda i, me: (i, 0, 0, 0, 0)),
        band,
        pl.BlockSpec(pot.shape, lambda i, me: (0, 0, 0)),
    ]
    args, aliases = [me, kin, wave, pot], {}
    if applied is not None:
        in_specs.append(pl.BlockSpec(memory_space=pl.ANY))
        args.append(applied)
        aliases = {4: 0}
    return pl.pallas_call(
        finish_kernel,
        grid_spec=pltpu.PrefetchScalarGridSpec(
            num_scalar_prefetch=1,
            grid=(count,),
            in_specs=in_specs,
            out_specs=[band, pl.BlockSpec((1, 8, 128), lambda i, me: (i ^ me[0], 0, 0))],
        ),
        out_shape=[
            jax.ShapeDtypeStruct(wave.shape, F32),
            jax.ShapeDtypeStruct((count, 8, 128), F32),
        ],
        input_output_aliases=aliases,
        compiler_params=pltpu.CompilerParams(**PARAMS),
    )(*args)


def exchange(value, axis):
    return lax.all_to_all(value, axis, split_axis=0, concat_axis=0, tiled=True)


def swap(pieces, axis):
    size = len(pieces)
    return jnp.stack(
        [pieces[0]]
        + [
            lax.ppermute(pieces[d], axis, [(i, i ^ d) for i in range(size)])
            for d in range(1, size)
        ]
    )


def merge(stats, axis):
    size = lax.axis_size(axis)
    every = exchange(jnp.broadcast_to(stats[None], (size,) + stats.shape), axis)
    norm, corr, rest = every[:, 0], every[:, 1], every[:, 2]
    norm_all, corr_all = jnp.sum(norm, axis=0), jnp.sum(corr, axis=0)
    gap = ratio_of(corr, norm) - ratio_of(corr_all, norm_all)[None]
    return jnp.stack([norm_all, corr_all, jnp.sum(rest + gap * gap * norm, axis=0)])


def ratio_of(corr, norm):
    return jnp.where(norm > 0.0, corr / jnp.where(norm > 0.0, norm, 1.0), 0.0)


def body(wavefunctions, potential, cutoff_sq, locked_mask):
    _, bands, rows_z, rows_y, n = wavefunctions.shape
    size_y, size_z = lax.axis_size("py"), lax.axis_size("pz")
    fh, fl = split_table(n, False)
    ih, il = split_table(n, True)
    fwd, inv = (fh, fl), (ih, il)
    fwd_t = (np.ascontiguousarray(fh.T), np.ascontiguousarray(fl.T))
    inv_t = (np.ascontiguousarray(ih.T), np.ascontiguousarray(il.T))
    order, rows, square, own = packing(n, size_z)
    share = rows // size_z
    both = np.concatenate([order, n + order])
    fwd_y, inv_y = (fh[both], fl[both]), (ih[:, both], il[:, both])
    squares = lax.dynamic_slice_in_dim(
        jnp.asarray(square)[:, None, :], lax.axis_index("pz") * share, share, 0
    )
    me = lax.axis_index("py").astype(jnp.int32)
    there, back = jnp.stack([me, 0 * me]), jnp.stack([0 * me, me])
    spectra = []
    gathered = None
    for first in range(0, bands, size_y):
        source = wavefunctions
        if gathered is not None:
            source, gathered = lax.optimization_barrier((source, gathered))
            spectra[-1] = gathered
        sent = [
            lax.dynamic_index_in_dim(source, first + (me ^ d), 1, keepdims=False)
            for d in range(size_y)
        ]
        gathered = swap(sent, "py")
        spectra.append(gathered)
    pieces = [
        planes_call(
            forward_kernel, there, fwd_y, fwd_t, own, x, (size_z, 2, share, rows_z, n), (2, 3)
        )
        for x in spectra
    ]
    pieces = [exchange(piece, "pz") for piece in pieces]
    pieces = [middle_call(cutoff_sq, squares, fwd, inv, x) for x in pieces]
    pieces = [exchange(piece, "pz") for piece in pieces]
    pieces = [
        planes_call(
            inverse_kernel, back, inv_y, inv_t, own, x, (size_y, 2, rows_z, rows_y, n), (3, 2)
        )
        for x in pieces
    ]
    applied, stats = None, []
    for index, piece in enumerate(pieces):
        kinetic_part = swap([piece[d] for d in range(size_y)], "py")
        applied, some = finish_call(
            me[None], kinetic_part, wavefunctions, potential, index * size_y, applied
        )
        stats.append(some[:, :3, 0])
    total = merge(merge(jnp.concatenate(stats, axis=0).T, "py"), "pz")
    rayleigh = total[1] / total[0]
    residual_norm = jnp.sqrt(total[2] / total[0]) * (1.0 - locked_mask.astype(F32))
    return (applied, rayleigh, residual_norm)


def solution(mesh):
    in_specs = (P(None, None, "pz", "py", None), P("pz", "py", None), P(), P())
    out_specs = (P(None, None, "pz", "py", None), P(), P())
    return jax.shard_map(body, mesh=mesh, in_specs=in_specs, out_specs=out_specs, check_vma=False)
```

```python
import math

import jax
import jax.numpy as jnp
import ml_dtypes
import numpy as np
from jax import lax
from jax.experimental import pallas as pl
from jax.experimental.pallas import tpu as pltpu
from jax.sharding import PartitionSpec as P

F32 = jnp.float32
BF16 = jnp.bfloat16


def split_table(length, inverse):
    counter = np.arange(length)
    angle = 2.0 * np.pi / length * (counter[:, None] * counter[None, :] % length)
    scale = 1.0 / length if inverse else 1.0
    sign = 1.0 if inverse else -1.0
    cosines, sines = scale * np.cos(angle), sign * scale * np.sin(angle)
    table = np.block([[cosines, -sines], [sines, cosines]]).astype(np.float32)
    high = table.astype(ml_dtypes.bfloat16)
    low = (table - high.astype(np.float32)).astype(ml_dtypes.bfloat16)
    return high, low


def split(value):
    high = value.astype(BF16)
    return high, (value - high.astype(F32)).astype(BF16)


def dot(left, right):
    return jnp.dot(left, right, preferred_element_type=F32)


def left_apply(high, low, value):
    vh, vl = split(value)
    return dot(high, vh) + (dot(high, vl) + dot(low, vh))


def right_apply(value, high, low):
    vh, vl = split(value)
    return dot(vh, high) + (dot(vl, high) + dot(vh, low))


def packing(n, owners):
    limit = n * n // 4
    signed = [k if k < n // 2 else k - n for k in range(n)]
    reach = [math.isqrt(limit - f * f) for f in signed]
    free, pairs = set(range(n)), []
    for tail in sorted(range(n), key=lambda k: reach[k]):
        fits = [k for k in free if k != tail and reach[k] + reach[tail] < n // 2]
        if tail in free and fits:
            host = max(fits, key=lambda k: reach[k])
            pairs.append((host, tail))
            free -= {host, tail}
    count = max(c for c in range(0, len(pairs) + 1, 8) if (n - c) % owners == 0)
    pairs = pairs[:count]
    used = {k for pair in pairs for k in pair}
    hosts, tails = [h for h, _ in pairs], [t for _, t in pairs]
    order = [k for k in range(n) if k not in used] + hosts + tails
    rows = n - count
    f = np.array(signed)
    square = (f[order[:rows], None] ** 2 + f[None, :] ** 2).astype(np.int32)
    own = np.ones((max(count, 8), n), np.int32)
    for i, (host, tail) in enumerate(pairs):
        lane = np.arange(n)
        own[i] = (lane <= reach[host]) | (lane >= n - reach[host])
        other = f[tail] ** 2 + np.roll(f, n // 2) ** 2
        square[rows - count + i] = np.where(own[i], square[rows - count + i], other)
    return np.array(order), rows, square, own


def gather_planes(planes):
    depth, n = len(planes), planes[0].shape[0]
    return lambda along: jnp.concatenate(
        [
            jnp.concatenate([along[z * n : (z + 1) * n, :n], along[z * n : (z + 1) * n, n:]], axis=0)
            for z in range(depth)
        ],
        axis=1,
    )


def forward_kernel(order, lh, ll, rh, rl, own, src, dst):
    pieces, _, depth, _, n = src.shape
    owners, _, share, _, _ = dst.shape
    rows = owners * share
    count = n - rows
    planes = []
    for z in range(depth):
        part = [
            jnp.concatenate([src[s ^ order[0], p, z] for s in range(pieces)], axis=0)
            for p in range(2)
        ]
        planes.append(jnp.concatenate(part, axis=1))
    along_x = right_apply(jnp.concatenate(planes, axis=0), rh[...], rl[...])
    out = left_apply(lh[...], ll[...], gather_planes(planes)(along_x))
    for q in range(2):
        packed = []
        for z in range(depth):
            plane = out[q * n : (q + 1) * n, z * n : (z + 1) * n]
            if count:
                tail = pltpu.roll(plane[rows:], n // 2, 1)
                host = jnp.where(own[...] != 0, plane[rows - count : rows], tail)
                plane = jnp.concatenate([plane[: rows - count], host], axis=0)
            packed.append(plane)
        packed = jnp.swapaxes(jnp.stack(packed, axis=0), 0, 1)
        dst[:, q] = packed.reshape(owners, share, depth, n)


def inverse_kernel(order, lh, ll, rh, rl, own, src, dst):
    owners, _, share, depth, n = src.shape
    pieces, _, _, width, _ = dst.shape
    rows = owners * share
    count = n - rows
    parts = [jnp.swapaxes(src[:, p].reshape(rows, depth, n), 0, 1) for p in range(2)]
    planes = []
    for z in range(depth):
        part = []
        for p in range(2):
            plane = parts[p][z]
            if count:
                last = plane[rows - count :]
                host = jnp.where(own[...] != 0, last, 0.0)
                tail = pltpu.roll(jnp.where(own[...] != 0, 0.0, last), n // 2, 1)
                plane = jnp.concatenate([plane[: rows - count], host, tail], axis=0)
            part.append(plane)
        planes.append(jnp.concatenate(part, axis=1))
    along_x = right_apply(jnp.concatenate(planes, axis=0), rh[...], rl[...])
    out = left_apply(lh[...], ll[...], gather_planes(planes)(along_x))
    for z in range(depth):
        for q in range(2):
            for d in range(pieces):
                first = q * n + d * width
                dst[d ^ order[1], q, z] = out[first : first + width, z * n : (z + 1) * n]


def middle_kernel(cutoff, squares, fh, fl, ih, il, src, dst):
    owners, _, width, depth, n = src.shape
    columns = jnp.concatenate(
        [
            jnp.concatenate([src[:, q, j].reshape(owners * depth, n) for q in range(2)], axis=0)
            for j in range(width)
        ],
        axis=1,
    )
    spectrum = left_apply(fh[...], fl[...], columns)
    kz = lax.broadcasted_iota(jnp.int32, (n, n), 0)
    kz = jnp.where(kz < n // 2, kz, kz - n)
    base = kz * kz
    kinetic = []
    for j in range(width):
        total = base + squares[j]
        value = (0.5 * (math.pi / n) ** 2) * total.astype(F32)
        kinetic.append(jnp.where(total <= cutoff[0], value, 0.0))
    kinetic = jnp.concatenate(kinetic, axis=1)
    kinetic = jnp.concatenate([kinetic, kinetic], axis=0)
    back = left_apply(ih[...], il[...], spectrum * kinetic)
    for q in range(2):
        for j in range(width):
            plane = back[q * n : (q + 1) * n, j * n : (j + 1) * n]
            dst[:, q, j] = plane.reshape(owners, depth, n)


def whole(shape):
    return pl.BlockSpec(shape, lambda i: (0,) * len(shape))


PARAMS = dict(dimension_semantics=("arbitrary",), vmem_limit_bytes=40 * 1024 * 1024)


def planes_call(kernel, order, left, right, own, src, out_shape, depths):
    n = src.shape[4]
    depth = math.gcd(src.shape[depths[0]], 8)

    def spec(shape, axis):
        block = shape[:axis] + (depth,) + shape[axis + 1 :]
        return pl.BlockSpec(block, lambda i: tuple(i if a == axis else 0 for a in range(5)))

    table = whole((2 * n, 2 * n))
    return pl.pallas_call(
        kernel,
        grid=(src.shape[depths[0]] // depth,),
        in_specs=[pl.BlockSpec(memory_space=pltpu.SMEM)]
        + [table] * 4
        + [whole(own.shape), spec(src.shape, depths[0])],
        out_specs=spec(out_shape, depths[1]),
        out_shape=jax.ShapeDtypeStruct(out_shape, F32),
        compiler_params=pltpu.CompilerParams(**PARAMS),
    )(order, *left, *right, own, src)


def middle_call(cutoff, squares, forward, inverse, src):
    owners, _, rows, depth, n = src.shape
    width = max(w for w in range(1, 9) if rows % w == 0)
    block = pl.BlockSpec((owners, 2, width, depth, n), lambda i: (0, 0, i, 0, 0))
    table = whole((2 * n, 2 * n))
    return pl.pallas_call(
        middle_kernel,
        grid=(rows // width,),
        in_specs=[
            pl.BlockSpec(memory_space=pltpu.SMEM),
            pl.BlockSpec((width, 1, n), lambda i: (i, 0, 0)),
        ]
        + [table] * 4
        + [block],
        out_specs=block,
        out_shape=jax.ShapeDtypeStruct(src.shape, F32),
        compiler_params=pltpu.CompilerParams(**PARAMS),
    )(cutoff, squares, *forward, *inverse, src)


def finish_kernel(me, kin, wave, pot, *refs):
    out, stats = refs[-2:]
    norm = corr = 0.0
    for p in range(2):
        w = wave[p, 0]
        a = kin[0, p] + pot[...] * w
        out[p, 0] = a
        norm = norm + jnp.sum(jnp.sum(w * w, axis=0), keepdims=True)
        corr = corr + jnp.sum(jnp.sum(w * a, axis=0), keepdims=True)
    ratio = jnp.where(norm > 0.0, corr / jnp.where(norm > 0.0, norm, 1.0), 0.0)
    rest = 0.0
    for p in range(2):
        gap = out[p, 0] - ratio[None] * wave[p, 0]
        rest = rest + jnp.sum(jnp.sum(gap * gap, axis=0), keepdims=True)
    row = lax.broadcasted_iota(jnp.int32, stats.shape[1:], 0)
    stats[0] = jnp.where(row == 0, norm, jnp.where(row == 1, corr, rest))


def finish_call(me, kin, wave, pot, first, applied):
    _, bands, depth, rows, n = wave.shape
    count = kin.shape[0]
    band = pl.BlockSpec((2, 1, depth, rows, n), lambda i, me: (0, first + (i ^ me[0]), 0, 0, 0))
    in_specs = [
        pl.BlockSpec((1, 2, depth, rows, n), lambda i, me: (i, 0, 0, 0, 0)),
        band,
        pl.BlockSpec(pot.shape, lambda i, me: (0, 0, 0)),
    ]
    args, aliases = [me, kin, wave, pot], {}
    if applied is not None:
        in_specs.append(pl.BlockSpec(memory_space=pl.ANY))
        args.append(applied)
        aliases = {4: 0}
    return pl.pallas_call(
        finish_kernel,
        grid_spec=pltpu.PrefetchScalarGridSpec(
            num_scalar_prefetch=1,
            grid=(count,),
            in_specs=in_specs,
            out_specs=[band, pl.BlockSpec((1, 8, 128), lambda i, me: (i ^ me[0], 0, 0))],
        ),
        out_shape=[
            jax.ShapeDtypeStruct(wave.shape, F32),
            jax.ShapeDtypeStruct((count, 8, 128), F32),
        ],
        input_output_aliases=aliases,
        compiler_params=pltpu.CompilerParams(**PARAMS),
    )(*args)


def exchange(value, axis):
    return lax.all_to_all(value, axis, split_axis=0, concat_axis=0, tiled=True)


def swap(pieces, axis):
    size = len(pieces)
    return jnp.stack(
        [pieces[0]]
        + [
            lax.ppermute(pieces[d], axis, [(i, i ^ d) for i in range(size)])
            for d in range(1, size)
        ]
    )


def merge(stats, axis):
    size = lax.axis_size(axis)
    every = exchange(jnp.broadcast_to(stats[None], (size,) + stats.shape), axis)
    norm, corr, rest = every[:, 0], every[:, 1], every[:, 2]
    norm_all, corr_all = jnp.sum(norm, axis=0), jnp.sum(corr, axis=0)
    gap = ratio_of(corr, norm) - ratio_of(corr_all, norm_all)[None]
    return jnp.stack([norm_all, corr_all, jnp.sum(rest + gap * gap * norm, axis=0)])


def ratio_of(corr, norm):
    return jnp.where(norm > 0.0, corr / jnp.where(norm > 0.0, norm, 1.0), 0.0)


def body(wavefunctions, potential, cutoff_sq, locked_mask):
    _, bands, rows_z, rows_y, n = wavefunctions.shape
    size_y, size_z = lax.axis_size("py"), lax.axis_size("pz")
    fh, fl = split_table(n, False)
    ih, il = split_table(n, True)
    fwd, inv = (fh, fl), (ih, il)
    fwd_t = (np.ascontiguousarray(fh.T), np.ascontiguousarray(fl.T))
    inv_t = (np.ascontiguousarray(ih.T), np.ascontiguousarray(il.T))
    order, rows, square, own = packing(n, size_z)
    share = rows // size_z
    both = np.concatenate([order, n + order])
    fwd_y, inv_y = (fh[both], fl[both]), (ih[:, both], il[:, both])
    squares = lax.dynamic_slice_in_dim(
        jnp.asarray(square)[:, None, :], lax.axis_index("pz") * share, share, 0
    )
    me = lax.axis_index("py").astype(jnp.int32)
    there, back = jnp.stack([me, 0 * me]), jnp.stack([0 * me, me])
    spectra = []
    gathered = None
    for first in range(0, bands, size_y):
        source = wavefunctions
        if gathered is not None:
            source, gathered = lax.optimization_barrier((source, gathered))
            spectra[-1] = gathered
        sent = [
            lax.dynamic_index_in_dim(source, first + (me ^ d), 1, keepdims=False)
            for d in range(size_y)
        ]
        gathered = swap(sent, "py")
        spectra.append(gathered)
    pieces = [
        planes_call(
            forward_kernel, there, fwd_y, fwd_t, own, x, (size_z, 2, share, rows_z, n), (2, 3)
        )
        for x in spectra
    ]
    pieces = [exchange(piece, "pz") for piece in pieces]
    pieces = [middle_call(cutoff_sq, squares, fwd, inv, x) for x in pieces]
    pieces = [exchange(piece, "pz") for piece in pieces]
    pieces = [
        planes_call(
            inverse_kernel, back, inv_y, inv_t, own, x, (size_y, 2, rows_z, rows_y, n), (3, 2)
        )
        for x in pieces
    ]
    applied, stats = None, []
    for index, piece in enumerate(pieces):
        kinetic_part = swap([piece[d] for d in range(size_y)], "py")
        applied, some = finish_call(
            me[None], kinetic_part, wavefunctions, potential, index * size_y, applied
        )
        stats.append(some[:, :3, 0])
    total = merge(jnp.concatenate(stats, axis=0).T, ("py", "pz"))
    rayleigh = total[1] / total[0]
    residual_norm = jnp.sqrt(total[2] / total[0]) * (1.0 - locked_mask.astype(F32))
    return (applied, rayleigh, residual_norm)


def solution(mesh):
    in_specs = (P(None, None, "pz", "py", None), P("pz", "py", None), P(), P())
    out_specs = (P(None, None, "pz", "py", None), P(), P())
    return jax.shard_map(body, mesh=mesh, in_specs=in_specs, out_specs=out_specs, check_vma=False)
```
